32 devices in a mesh: part: 2 (over x), tpa: 4 (over z), tpb: 4 (over y, core).
Axes of the slice: x: 2, y: 2, z: 4, core: 2. Of those that a mesh axis runs over, the one named last changes fastest.
Arguments:
- x: bfloat16 [32, 1024, 3072], P(('part', 'tpb')), parts along dimension 0
- lengths: int32 [32], P(('part', 'tpb')), parts along dimension 0
- k_buf: bfloat16 [32, 1024, 8, 128], P(('part', 'tpb'), None, 'tpa'), parts along dimension 0
- v_buf: bfloat16 [32, 1024, 8, 128], P(('part', 'tpb'), None, 'tpa'), parts along dimension 0
- w_qkv: bfloat16 [6144, 5120], P('part', ('tpa', 'tpb')), parts along dimension 0
- w_o: bfloat16 [6144, 3072], P(('part', 'tpa', 'tpb')), parts along dimension 0
- w_gate_up: bfloat16 [6144, 16384], P('part', ('tpa', 'tpb')), parts along dimension 0
- w_down: bfloat16 [16384, 3072], P(('part', 'tpa', 'tpb')), parts along dimension 0
- g_attn: bfloat16 [6144], P('part'), parts along dimension 0
- g_mlp: bfloat16 [6144], P('part'), parts along dimension 0
Outputs:
- output 1: bfloat16 [32, 1024, 3072], P(('part', 'tpb')), parts along dimension 0
- output 2: bfloat16 [32, 1024, 8, 128], P(('part', 'tpb'), None, 'tpa'), parts along dimension 0
- output 3: bfloat16 [32, 1024, 8, 128], P(('part', 'tpb'), None, 'tpa'), parts along dimension 0
- output 4: bfloat16 [6144, 3072], P('part', 'tpa'), parts along dimension 0
- output 5: bfloat16 [6144, 1024], P('part', 'tpa'), parts along dimension 0
- output 6: bfloat16 [6144, 1024], P('part', 'tpa'), parts along dimension 0
- output 7: bfloat16 [6144, 3072], P(('part', 'tpa')), parts along dimension 0
- output 8: bfloat16 [6144, 8192], P('part', 'tpa'), parts along dimension 0
- output 9: bfloat16 [6144, 8192], P('part', 'tpa'), parts along dimension 0
- output 10: bfloat16 [16384, 3072], P(('part', 'tpa')), parts along dimension 0
There are 2 independent parts. The reference program is written for one: setup_inputs(seed, part) draws one part's arguments, and reference() takes and returns one part's arrays. A program takes and returns all parts, laid end to end along the dimension named above; each array names one.
All inputs are finite; a program needn't handle non-finite values.
Results may differ from the reference program's by a relative error of at most 0.0138525.
Values are sent between devices in bfloat16 or wider.
A program may use at most 1 GiB of HBM per device.

```python
import math
import jax
import jax.numpy as jnp
from jax import lax

D = 3072
HEADS = 24
KV_HEADS = 8
HEAD = 128
FF = 8192
BATCH = 16
SEQ = 1024
TRAIN_TP = 16
GROUP = HEADS // KV_HEADS
QKV_COLS = KV_HEADS * (GROUP + 2) * HEAD
FF_BLOCK = FF // TRAIN_TP
ROPE_BASE = 500000.0
ROPE_FACTOR = 8.0
LOW_FREQ = 1.0
HIGH_FREQ = 4.0
ORIG_CONTEXT = 8192.0
NORM_EPS = 1e-5
MASK_VALUE = -1e30


def setup_inputs(seed: int = 0, part: int = 0) -> dict:
    part_key = jax.random.fold_in(jax.random.key(seed), part)
    sub_keys = jax.random.split(part_key, 10)
    x_in = jax.random.normal(sub_keys[0], (BATCH, SEQ, D), jnp.float32)
    drawn_len = jax.random.randint(sub_keys[1], (BATCH,), 1, SEQ + 1)
    lengths = jnp.where(jnp.arange(BATCH) == 0, SEQ, drawn_len).astype(jnp.int32)
    k_buf = jax.random.normal(sub_keys[2], (BATCH, SEQ, KV_HEADS, HEAD), jnp.float32)
    v_buf = jax.random.normal(sub_keys[3], (BATCH, SEQ, KV_HEADS, HEAD), jnp.float32)
    qk_scale = jnp.where(jnp.arange(GROUP + 2) <= GROUP, 1.5, 1.0)[:, None]
    w_qkv = (jax.random.normal(sub_keys[4], (D, KV_HEADS, GROUP + 2, HEAD), jnp.float32) * qk_scale * D ** -0.5).reshape(D, QKV_COLS)
    w_o = jax.random.normal(sub_keys[5], (HEADS * HEAD, D), jnp.float32) * (HEADS * HEAD) ** -0.5
    w_gate_up = jax.random.normal(sub_keys[6], (D, 2 * FF), jnp.float32) * D ** -0.5
    w_down = jax.random.normal(sub_keys[7], (FF, D), jnp.float32) * FF ** -0.5
    g_attn = 1.0 + 0.4 * jax.random.normal(sub_keys[8], (D,), jnp.float32)
    g_mlp = 1.0 + 0.4 * jax.random.normal(sub_keys[9], (D,), jnp.float32)
    return {'x': x_in.astype(jnp.bfloat16), 'lengths': lengths, 'k_buf': k_buf.astype(jnp.bfloat16), 'v_buf': v_buf.astype(jnp.bfloat16), 'w_qkv': w_qkv.astype(jnp.bfloat16), 'w_o': w_o.astype(jnp.bfloat16), 'w_gate_up': w_gate_up.astype(jnp.bfloat16), 'w_down': w_down.astype(jnp.bfloat16), 'g_attn': g_attn.astype(jnp.bfloat16), 'g_mlp': g_mlp.astype(jnp.bfloat16)}


def rms_norm(x_in, gain_vec):
    x_wide = x_in.astype(jnp.float32)
    mean_sq = jnp.mean(x_wide * x_wide, axis=-1, keepdims=True)
    return (x_wide * lax.rsqrt(mean_sq + NORM_EPS) * gain_vec.astype(jnp.float32)).astype(jnp.bfloat16)


def rope_tables():
    exponent = jnp.arange(HEAD // 2, dtype=jnp.float32) * (2.0 / HEAD)
    inv_freq = 1.0 / jnp.power(ROPE_BASE, exponent)
    wavelen = 2.0 * math.pi / inv_freq
    smooth = (ORIG_CONTEXT / wavelen - LOW_FREQ) / (HIGH_FREQ - LOW_FREQ)
    blended = (1.0 - smooth) * inv_freq / ROPE_FACTOR + smooth * inv_freq
    rope_freq = jnp.where(wavelen < ORIG_CONTEXT / HIGH_FREQ, inv_freq, jnp.where(wavelen > ORIG_CONTEXT / LOW_FREQ, inv_freq / ROPE_FACTOR, blended))
    angles = jnp.arange(SEQ, dtype=jnp.float32)[:, None] * rope_freq[None, :]
    return jnp.cos(angles), jnp.sin(angles)


def apply_rope(vec_in, cos_tab, sin_tab):
    half_dim = vec_in.shape[-1] // 2
    first_half = vec_in[..., :half_dim]
    second_half = vec_in[..., half_dim:]
    return jnp.concatenate([first_half * cos_tab - second_half * sin_tab, second_half * cos_tab + first_half * sin_tab], axis=-1)


def reference(x, lengths, k_buf, v_buf, w_qkv, w_o, w_gate_up, w_down, g_attn, g_mlp):
    packed = w_qkv.reshape(D, KV_HEADS, GROUP + 2, HEAD)
    w_q = packed[:, :, :GROUP, :].reshape(D, HEADS * HEAD)
    w_k = packed[:, :, GROUP, :].reshape(D, KV_HEADS * HEAD)
    w_v = packed[:, :, GROUP + 1, :].reshape(D, KV_HEADS * HEAD)
    gu_view = w_gate_up.reshape(D, TRAIN_TP, 2, FF_BLOCK)
    w_gate = gu_view[:, :, 0, :].reshape(D, FF)
    w_up = gu_view[:, :, 1, :].reshape(D, FF)
    cos_tab, sin_tab = rope_tables()
    positions = jnp.arange(SEQ)
    causal = positions[None, :] <= positions[:, None]

    def one_prompt(prompt_item):
        tokens, length = prompt_item
        x_normed = rms_norm(tokens, g_attn)
        queries = jnp.dot(x_normed, w_q, preferred_element_type=jnp.float32).astype(jnp.bfloat16).reshape(SEQ, KV_HEADS, GROUP, HEAD)
        keys_new = jnp.dot(x_normed, w_k, preferred_element_type=jnp.float32).astype(jnp.bfloat16).reshape(SEQ, KV_HEADS, HEAD)
        values = jnp.dot(x_normed, w_v, preferred_element_type=jnp.float32).astype(jnp.bfloat16).reshape(SEQ, KV_HEADS, HEAD)
        q_rot = apply_rope(queries.astype(jnp.float32), cos_tab[:, None, None, :], sin_tab[:, None, None, :]).astype(jnp.bfloat16)
        k_rot = apply_rope(keys_new.astype(jnp.float32), cos_tab[:, None, :], sin_tab[:, None, :]).astype(jnp.bfloat16)
        allowed = causal & (positions[None, :] < length)

        def one_group(kv_item):
            q_head, k_head, v_head = kv_item
            scores = jnp.einsum('qgd,sd->gqs', q_head.astype(jnp.float32), k_head.astype(jnp.float32)) * HEAD ** -0.5
            scores = jnp.where(allowed[None], scores, MASK_VALUE)
            attn_prob = jax.nn.softmax(scores, axis=-1).astype(jnp.bfloat16)
            return jnp.einsum('gqs,sd->qgd', attn_prob.astype(jnp.float32), v_head.astype(jnp.float32)).astype(jnp.bfloat16)

        per_group = lax.map(one_group, (q_rot.transpose(1, 0, 2, 3), k_rot.transpose(1, 0, 2), values.transpose(1, 0, 2)))
        attn_out = per_group.transpose(1, 0, 2, 3).reshape(SEQ, HEADS * HEAD)
        attn_proj = jnp.dot(attn_out, w_o, preferred_element_type=jnp.float32)
        hidden = (tokens.astype(jnp.float32) + attn_proj).astype(jnp.bfloat16)
        h_normed = rms_norm(hidden, g_mlp)
        gate_act = jnp.dot(h_normed, w_gate, preferred_element_type=jnp.float32).astype(jnp.bfloat16)
        up_act = jnp.dot(h_normed, w_up, preferred_element_type=jnp.float32).astype(jnp.bfloat16)
        mid_act = (jax.nn.silu(gate_act.astype(jnp.float32)) * up_act.astype(jnp.float32)).astype(jnp.bfloat16)
        layer_out = (hidden.astype(jnp.float32) + jnp.dot(mid_act, w_down, preferred_element_type=jnp.float32)).astype(jnp.bfloat16)
        return layer_out, k_rot, values

    layer_out, k_new, v_new = lax.map(one_prompt, (x, lengths))
    valid_pos = (positions[None, :] < lengths[:, None])[:, :, None, None]
    k_cache = jnp.where(valid_pos, k_new, k_buf)
    v_cache = jnp.where(valid_pos, v_new, v_buf)
    return (layer_out, k_cache, v_cache, w_q, w_k, w_v, w_o, w_gate, w_up, w_down)
```

```python
import math
import jax
import jax.numpy as jnp
from jax import lax
from jax.experimental import pallas as pl
from jax.sharding import PartitionSpec as P

ROPE_BASE = 500000.0
ROPE_FACTOR = 8.0
LOW_FREQ = 1.0
HIGH_FREQ = 4.0
ORIG_CONTEXT = 8192.0
NORM_EPS = 1e-5
MASK_VALUE = -1e30


def rms_norm(x_in, gain_vec):
    x_wide = x_in.astype(jnp.float32)
    mean_sq = jnp.mean(x_wide * x_wide, axis=-1, keepdims=True)
    return (x_wide * lax.rsqrt(mean_sq + NORM_EPS) * gain_vec.astype(jnp.float32)).astype(jnp.bfloat16)


def rope_tables(seq_len, head_dim):
    exponent = jnp.arange(head_dim // 2, dtype=jnp.float32) * (2.0 / head_dim)
    inv_freq = 1.0 / jnp.power(ROPE_BASE, exponent)
    wavelen = 2.0 * math.pi / inv_freq
    smooth = (ORIG_CONTEXT / wavelen - LOW_FREQ) / (HIGH_FREQ - LOW_FREQ)
    blended = (1.0 - smooth) * inv_freq / ROPE_FACTOR + smooth * inv_freq
    rope_freq = jnp.where(wavelen < ORIG_CONTEXT / HIGH_FREQ, inv_freq, jnp.where(wavelen > ORIG_CONTEXT / LOW_FREQ, inv_freq / ROPE_FACTOR, blended))
    angles = jnp.arange(seq_len, dtype=jnp.float32)[:, None] * rope_freq[None, :]
    return jnp.cos(angles), jnp.sin(angles)


def apply_rope(vec_in, cos_tab, sin_tab):
    half_dim = vec_in.shape[-1] // 2
    first_half = vec_in[..., :half_dim]
    second_half = vec_in[..., half_dim:]
    return jnp.concatenate([first_half * cos_tab - second_half * sin_tab, second_half * cos_tab + first_half * sin_tab], axis=-1)


ROW_SPLIT = 2


def split_qkv(qkv_cols, kv_local, head_dim):
    model_dim = qkv_cols.shape[0]
    group_size = qkv_cols.shape[1] // (kv_local * head_dim) - 2
    packed = qkv_cols.reshape(model_dim, kv_local, group_size + 2, head_dim)
    w_query = packed[:, :, :group_size, :].reshape(model_dim, kv_local * group_size * head_dim)
    w_key = packed[:, :, group_size, :].reshape(model_dim, kv_local * head_dim)
    w_value = packed[:, :, group_size + 1, :].reshape(model_dim, kv_local * head_dim)
    return w_query, w_key, w_value


def dot_f32(lhs, rhs):
    return jnp.dot(lhs, rhs, preferred_element_type=jnp.float32)


def add_bf16(a, b):
    return lax.reduce_precision(a.astype(jnp.float32) + b.astype(jnp.float32), 8, 7).astype(jnp.bfloat16)


def inward(part, axis):
    return lax.ppermute(part, axis, [(0, 1), (3, 2)])


def across(part, axis):
    return lax.ppermute(part, axis, [(1, 2), (2, 1)])


def outward(total, axis):
    got = lax.ppermute(total, axis, [(1, 0), (2, 3)])
    place = lax.axis_index(axis)
    return jnp.where((place == 0) | (place == 3), got, total)


tie = lax.optimization_barrier


def settle(array):
    rows, cols = array.shape
    block = pl.BlockSpec((min(rows, 256), cols), lambda i: (i, 0))

    def body(src_ref, dst_ref):
        dst_ref[...] = src_ref[...]

    return pl.pallas_call(body, grid=(rows // min(rows, 256),), in_specs=[block], out_specs=block, out_shape=jax.ShapeDtypeStruct(array.shape, array.dtype), cost_estimate=pl.CostEstimate(flops=10**9, bytes_accessed=4 * rows * cols, transcendentals=0))(array)


def line_items(n_chunks, rows):
    items = [('attn', c, 0, rows) for c in range(n_chunks)]
    for c in range(n_chunks):
        pieces = {n_chunks - 1: 4, n_chunks - 2: 2}.get(c, 1)
        items += [('mlp', c, i, rows // pieces) for i in range(0, rows, rows // pieces)]
    return items


def attention(x_prompt, length, qkv_cols, o_rows, g_attn, cos_tab, sin_tab, kv_local, head_dim):
    seq_len = x_prompt.shape[0]
    group_size = qkv_cols.shape[1] // (kv_local * head_dim) - 2
    qkv_act = dot_f32(rms_norm(x_prompt, g_attn), qkv_cols).astype(jnp.bfloat16)
    qkv_act = qkv_act.reshape(seq_len, kv_local, group_size + 2, head_dim)
    q_rot = apply_rope(qkv_act[:, :, :group_size, :].astype(jnp.float32), cos_tab[:, None, None, :], sin_tab[:, None, None, :]).astype(jnp.bfloat16)
    k_rot = apply_rope(qkv_act[:, :, group_size, :].astype(jnp.float32), cos_tab[:, None, :], sin_tab[:, None, :]).astype(jnp.bfloat16)
    values = qkv_act[:, :, group_size + 1, :]
    scores = jnp.einsum('qkgd,skd->kgqs', q_rot, k_rot, preferred_element_type=jnp.float32) * head_dim ** -0.5
    positions = jnp.arange(seq_len)
    allowed = (positions[None, :] <= positions[:, None]) & (positions[None, :] < length)
    scores = jnp.where(allowed[None, None], scores, MASK_VALUE)
    attn_prob = jax.nn.softmax(scores, axis=-1).astype(jnp.bfloat16)
    attn_out = jnp.einsum('kgqs,skd->qkgd', attn_prob, values, preferred_element_type=jnp.float32).astype(jnp.bfloat16)
    attn_out = attn_out.reshape(seq_len, kv_local * group_size * head_dim)
    return dot_f32(attn_out, o_rows).astype(jnp.bfloat16), k_rot, values


def mlp(hidden, w_gate, w_up, down_rows, g_mlp):
    h_normed = rms_norm(hidden, g_mlp)
    gate_act = dot_f32(h_normed, w_gate).astype(jnp.bfloat16)
    up_act = dot_f32(h_normed, w_up).astype(jnp.bfloat16)
    mid_act = (jax.nn.silu(gate_act.astype(jnp.float32)) * up_act.astype(jnp.float32)).astype(jnp.bfloat16)
    return dot_f32(mid_act, down_rows).astype(jnp.bfloat16)


def residual(base, delta):
    return (base.astype(jnp.float32) + delta.astype(jnp.float32)).astype(jnp.bfloat16)


def solution(mesh):
    assert mesh.shape['tpa'] == 4

    def one_layer(x_loc, len_loc, k_buf, v_buf, w_qkv, w_o, w_gate_up, w_down, g_attn, g_mlp):
        batch_loc, seq_len, _ = x_loc.shape
        kv_local, head_dim = k_buf.shape[2], k_buf.shape[3]
        ff_block = w_gate_up.shape[1] // 2
        qkv_cols = lax.all_gather(w_qkv, 'tpb', axis=1, tiled=True)
        w_o, qkv_cols = lax.optimization_barrier((w_o, qkv_cols))
        o_rows = lax.all_gather(w_o, 'tpb', axis=0, tiled=True)
        w_gate_up, o_rows = lax.optimization_barrier((w_gate_up, o_rows))
        w_gate = lax.all_gather(w_gate_up[:, :ff_block], 'tpb', axis=1, tiled=True)
        w_up = lax.all_gather(w_gate_up[:, ff_block:], 'tpb', axis=1, tiled=True)
        w_down, w_up = lax.optimization_barrier((w_down, w_up))
        down_rows = lax.all_gather(w_down, 'tpb', axis=0, tiled=True)
        cos_tab, sin_tab = rope_tables(seq_len, head_dim)
        layer_out = jnp.zeros_like(x_loc)
        rows = seq_len // ROW_SPLIT
        k_new, v_new = [], []
        chunks = [(b, r) for b in range(batch_loc) for r in range(0, seq_len, rows)]
        n_chunks = len(chunks)
        items = line_items(n_chunks, rows)
        n_items = len(items)
        first, total, mlp_part, hidden = {}, {}, {}, {}
        waiting, settled = {'o': o_rows, 'gate': w_gate, 'up': w_up, 'down': down_rows}, {}
        x_prompt = {b: x_loc[b] for b in range(batch_loc)}
        attn_part = None
        for t in range(n_items + 2):
            if t < n_items:
                kind, c, start, size = items[t]
                if kind == 'attn':
                    b, r = chunks[c]
                    if r == 0:
                        attn_part, k_rot, values = attention(x_prompt[b], len_loc[b], qkv_cols, o_rows, g_attn, cos_tab, sin_tab, kv_local, head_dim)
                        if b + 1 < batch_loc:
                            x_prompt[b + 1], attn_part, k_rot, values = tie((x_prompt[b + 1], attn_part, k_rot, values))
                        k_new.append(k_rot)
                        v_new.append(values)
                    part = attn_part[r:r + rows]
                else:
                    part = mlp_part[c][start:start + size]
                got = inward(part, 'tpa')
            if t >= 1 and t - 1 < n_items:
                if t < n_items:
                    if t + 1 < batch_loc:
                        part, first[t - 1], x_prompt[t + 1] = tie((part, first[t - 1], x_prompt[t + 1]))
                    else:
                        part, first[t - 1] = tie((part, first[t - 1]))
                crossed = across(first[t - 1], 'tpa')
                total_next = add_bf16(first[t - 1], crossed)
            if t >= 2:
                if t < n_items:
                    part, total[t - 2] = tie((part, total[t - 2]))
                kind, c, start, size = items[t - 2]
                b, r = chunks[c]
                summed = outward(total[t - 2], 'tpa')
                if kind == 'attn':
                    x_rows, summed = tie((x_loc[b, r:r + rows], summed))
                    hidden[c] = residual(x_rows, summed)
                    mlp_part[c] = mlp(hidden[c], w_gate, w_up, down_rows, g_mlp)
                else:
                    piece = residual(hidden[c][start:start + size], summed)
                    layer_out = lax.dynamic_update_slice(layer_out, piece[None], (b, r + start, 0))
            if 3 <= t < n_items and items[t - 3][0] == 'attn':
                c = items[t - 3][1]
                part, mlp_part[c] = tie((part, mlp_part[c]))
                name = {2: 'o', 3: 'gate', 4: 'up', 5: 'down'}.get(c)
                if name:
                    waiting[name], mlp_part[c] = tie((waiting[name], mlp_part[c]))
                    settled[name] = settle(waiting[name])
                    part, settled[name] = tie((part, settled[name]))
                if c == n_chunks - 3:
                    qkv_cols, mlp_part[c] = tie((qkv_cols, mlp_part[c]))
            if t < n_items:
                first[t] = add_bf16(part, got)
            if t >= 1 and t - 1 < n_items:
                total[t - 1] = total_next
        valid_pos = (jnp.arange(seq_len)[None, :] < len_loc[:, None])[:, :, None, None]
        k_cache = jnp.where(valid_pos, jnp.stack(k_new), k_buf)
        v_cache = jnp.where(valid_pos, jnp.stack(v_new), v_buf)
        w_query, w_key, w_value = split_qkv(qkv_cols, kv_local, head_dim)
        return (layer_out, k_cache, v_cache, w_query, w_key, w_value, settled['o'], settled['gate'], settled['up'], settled['down'])

    batch_spec = P(('part', 'tpb'), None, None)
    len_spec = P(('part', 'tpb'))
    cache_spec = P(('part', 'tpb'), None, 'tpa', None)
    train_cols = P('part', ('tpa', 'tpb'))
    train_rows = P(('part', 'tpa', 'tpb'), None)
    gain_spec = P('part')
    gen_cols = P('part', 'tpa')
    gen_rows = P(('part', 'tpa'), None)
    return jax.shard_map(one_layer, mesh=mesh, in_specs=(batch_spec, len_spec, cache_spec, cache_spec, train_cols, train_rows, train_cols, train_rows, gain_spec, gain_spec), out_specs=(batch_spec, cache_spec, cache_spec, gen_cols, gen_cols, gen_cols, gen_rows, gen_cols, gen_cols, gen_rows), check_vma=False)
```

```python
import math
import jax
import jax.numpy as jnp
from jax import lax
from jax.experimental import pallas as pl
from jax.sharding import PartitionSpec as P

ROPE_BASE = 500000.0
ROPE_FACTOR = 8.0
LOW_FREQ = 1.0
HIGH_FREQ = 4.0
ORIG_CONTEXT = 8192.0
NORM_EPS = 1e-5
MASK_VALUE = -1e30


def rms_norm(x_in, gain_vec):
    x_wide = x_in.astype(jnp.float32)
    mean_sq = jnp.mean(x_wide * x_wide, axis=-1, keepdims=True)
    return (x_wide * lax.rsqrt(mean_sq + NORM_EPS) * gain_vec.astype(jnp.float32)).astype(jnp.bfloat16)


def rope_tables(seq_len, head_dim):
    exponent = jnp.arange(head_dim // 2, dtype=jnp.float32) * (2.0 / head_dim)
    inv_freq = 1.0 / jnp.power(ROPE_BASE, exponent)
    wavelen = 2.0 * math.pi / inv_freq
    smooth = (ORIG_CONTEXT / wavelen - LOW_FREQ) / (HIGH_FREQ - LOW_FREQ)
    blended = (1.0 - smooth) * inv_freq / ROPE_FACTOR + smooth * inv_freq
    rope_freq = jnp.where(wavelen < ORIG_CONTEXT / HIGH_FREQ, inv_freq, jnp.where(wavelen > ORIG_CONTEXT / LOW_FREQ, inv_freq / ROPE_FACTOR, blended))
    angles = jnp.arange(seq_len, dtype=jnp.float32)[:, None] * rope_freq[None, :]
    return jnp.cos(angles), jnp.sin(angles)


def apply_rope(vec_in, cos_tab, sin_tab):
    half_dim = vec_in.shape[-1] // 2
    first_half = vec_in[..., :half_dim]
    second_half = vec_in[..., half_dim:]
    return jnp.concatenate([first_half * cos_tab - second_half * sin_tab, second_half * cos_tab + first_half * sin_tab], axis=-1)


ROW_SPLIT = 2
MLP_LATER = 2


def split_qkv(qkv_cols, kv_local, head_dim):
    model_dim = qkv_cols.shape[0]
    group_size = qkv_cols.shape[1] // (kv_local * head_dim) - 2
    packed = qkv_cols.reshape(model_dim, kv_local, group_size + 2, head_dim)
    w_query = packed[:, :, :group_size, :].reshape(model_dim, kv_local * group_size * head_dim)
    w_key = packed[:, :, group_size, :].reshape(model_dim, kv_local * head_dim)
    w_value = packed[:, :, group_size + 1, :].reshape(model_dim, kv_local * head_dim)
    return w_query, w_key, w_value


def dot_f32(lhs, rhs):
    return jnp.dot(lhs, rhs, preferred_element_type=jnp.float32)


def add_bf16(a, b):
    return lax.reduce_precision(a.astype(jnp.float32) + b.astype(jnp.float32), 8, 7).astype(jnp.bfloat16)


def inward(part, axis):
    return lax.ppermute(part, axis, [(0, 1), (3, 2)])


def across(part, axis):
    return lax.ppermute(part, axis, [(1, 2), (2, 1)])


def outward(total, axis):
    got = lax.ppermute(total, axis, [(1, 0), (2, 3)])
    place = lax.axis_index(axis)
    return jnp.where((place == 0) | (place == 3), got, total)


tie = lax.optimization_barrier


def settle(array):
    rows, cols = array.shape
    block = pl.BlockSpec((min(rows, 256), cols), lambda i: (i, 0))

    def body(src_ref, dst_ref):
        dst_ref[...] = src_ref[...]

    return pl.pallas_call(body, grid=(rows // min(rows, 256),), in_specs=[block], out_specs=block, out_shape=jax.ShapeDtypeStruct(array.shape, array.dtype), cost_estimate=pl.CostEstimate(flops=10**9, bytes_accessed=4 * rows * cols, transcendentals=0))(array)


def line_items(n_chunks, rows):
    items = [('attn', c, 0, rows) for c in range(n_chunks)]
    for c in range(n_chunks):
        pieces = {n_chunks - 1: 4, n_chunks - 2: 2}.get(c, 1)
        items += [('mlp', c, i, rows // pieces) for i in range(0, rows, rows // pieces)]
    return items


def attention(qkv_act, length, o_rows, cos_tab, sin_tab, kv_local, head_dim):
    seq_len = qkv_act.shape[0]
    group_size = qkv_act.shape[1] // (kv_local * head_dim) - 2
    qkv_act = qkv_act.reshape(seq_len, kv_local, group_size + 2, head_dim)
    q_rot = apply_rope(qkv_act[:, :, :group_size, :].astype(jnp.float32), cos_tab[:, None, None, :], sin_tab[:, None, None, :]).astype(jnp.bfloat16)
    k_rot = apply_rope(qkv_act[:, :, group_size, :].astype(jnp.float32), cos_tab[:, None, :], sin_tab[:, None, :]).astype(jnp.bfloat16)
    values = qkv_act[:, :, group_size + 1, :]
    scores = jnp.einsum('qkgd,skd->kgqs', q_rot, k_rot, preferred_element_type=jnp.float32) * head_dim ** -0.5
    positions = jnp.arange(seq_len)
    allowed = (positions[None, :] <= positions[:, None]) & (positions[None, :] < length)
    scores = jnp.where(allowed[None, None], scores, MASK_VALUE)
    attn_prob = jax.nn.softmax(scores, axis=-1).astype(jnp.bfloat16)
    attn_out = jnp.einsum('kgqs,skd->qkgd', attn_prob, values, preferred_element_type=jnp.float32).astype(jnp.bfloat16)
    attn_out = attn_out.reshape(seq_len, kv_local * group_size * head_dim)
    return dot_f32(attn_out, o_rows).astype(jnp.bfloat16), k_rot, values


def mlp(hidden, w_gate, w_up, down_rows, g_mlp):
    h_normed = rms_norm(hidden, g_mlp)
    gate_act = dot_f32(h_normed, w_gate).astype(jnp.bfloat16)
    up_act = dot_f32(h_normed, w_up).astype(jnp.bfloat16)
    mid_act = (jax.nn.silu(gate_act.astype(jnp.float32)) * up_act.astype(jnp.float32)).astype(jnp.bfloat16)
    return dot_f32(mid_act, down_rows).astype(jnp.bfloat16)


def residual(base, delta):
    return (base.astype(jnp.float32) + delta.astype(jnp.float32)).astype(jnp.bfloat16)


def solution(mesh):
    assert mesh.shape['tpa'] == 4

    def one_layer(x_loc, len_loc, k_buf, v_buf, w_qkv, w_o, w_gate_up, w_down, g_attn, g_mlp):
        batch_loc, seq_len, _ = x_loc.shape
        kv_local, head_dim = k_buf.shape[2], k_buf.shape[3]
        ff_block = w_gate_up.shape[1] // 2
        qkv_cols = lax.all_gather(w_qkv, 'tpb', axis=1, tiled=True)
        w_o, qkv_cols = lax.optimization_barrier((w_o, qkv_cols))
        o_rows = lax.all_gather(w_o, 'tpb', axis=0, tiled=True)
        qkv_first = dot_f32(rms_norm(x_loc[0], g_attn), qkv_cols).astype(jnp.bfloat16)
        w_gate_up, qkv_first = tie((w_gate_up, qkv_first))
        w_gate = lax.all_gather(w_gate_up[:, :ff_block], 'tpb', axis=1, tiled=True)
        w_up = lax.all_gather(w_gate_up[:, ff_block:], 'tpb', axis=1, tiled=True)
        w_down, qkv_first = tie((w_down, qkv_first))
        down_rows = lax.all_gather(w_down, 'tpb', axis=0, tiled=True)
        cos_tab, sin_tab = rope_tables(seq_len, head_dim)
        layer_out = jnp.zeros_like(x_loc)
        rows = seq_len // ROW_SPLIT
        k_new, v_new = [], []
        chunks = [(b, r) for b in range(batch_loc) for r in range(0, seq_len, rows)]
        n_chunks = len(chunks)
        items = line_items(n_chunks, rows)
        n_items = len(items)
        first, total, mlp_part, hidden = {}, {}, {}, {}
        waiting, settled = {'o': o_rows, 'gate': w_gate, 'up': w_up, 'down': down_rows}, {}
        cols_of = {b: qkv_cols for b in range(batch_loc)}
        summed = {}
        attn_part = None
        for t in range(n_items + 2):
            if t < n_items:
                kind, c, start, size = items[t]
                if kind == 'attn':
                    b, r = chunks[c]
                    if r == 0:
                        qkv_act = qkv_first
                        if b:
                            qkv_act = dot_f32(rms_norm(x_loc[b], g_attn), cols_of[b]).astype(jnp.bfloat16)
                        attn_part, k_rot, values = attention(qkv_act, len_loc[b], o_rows, cos_tab, sin_tab, kv_local, head_dim)
                        if b + 1 < batch_loc:
                            cols_of[b + 1], attn_part, k_rot, values = tie((cols_of[b + 1], attn_part, k_rot, values))
                        k_new.append(k_rot)
                        v_new.append(values)
                    part = attn_part[r:r + rows]
                else:
                    part = mlp_part[c][start:start + size]
                got = inward(part, 'tpa')
            if t >= 1 and t - 1 < n_items:
                if t < n_items:
                    if t + 1 < batch_loc:
                        part, first[t - 1], cols_of[t + 1] = tie((part, first[t - 1], cols_of[t + 1]))
                    else:
                        part, first[t - 1] = tie((part, first[t - 1]))
                crossed = across(first[t - 1], 'tpa')
                total_next = add_bf16(first[t - 1], crossed)
            if 2 <= t < n_items + 2:
                if t < n_items:
                    part, total[t - 2] = tie((part, total[t - 2]))
                kind, c, start, size = items[t - 2]
                b, r = chunks[c]
                out = outward(total[t - 2], 'tpa')
                if kind == 'attn':
                    summed[c] = out
                else:
                    piece = residual(hidden[c][start:start + size], out)
                    layer_out = lax.dynamic_update_slice(layer_out, piece[None], (b, r + start, 0))
            c = t - 2 - MLP_LATER
            if c in summed:
                b, r = chunks[c]
                if c:
                    summed[c], mlp_part[c - 1] = tie((summed[c], mlp_part[c - 1]))
                hidden[c] = residual(x_loc[b, r:r + rows], summed[c])
                mlp_part[c] = mlp(hidden[c], w_gate, w_up, down_rows, g_mlp)
            c = t - 3 - MLP_LATER
            if c in mlp_part:
                part, mlp_part[c] = tie((part, mlp_part[c]))
            if t < n_items:
                for name in list(settled):
                    part, settled[name] = tie((part, settled[name]))
                name = {n_chunks + 3: 'o', n_chunks + 4: 'gate', n_chunks + 5: 'up', n_chunks + 6: 'down'}.get(t)
                if name:
                    waiting[name], total[t - 2] = tie((waiting[name], total[t - 2]))
                    settled[name] = settle(waiting[name])
                if t == n_chunks + 2:
                    qkv_cols, total[t - 2] = tie((qkv_cols, total[t - 2]))
            if t < n_items:
                first[t] = add_bf16(part, got)
            if t >= 1 and t - 1 < n_items:
                total[t - 1] = total_next
        valid_pos = (jnp.arange(seq_len)[None, :] < len_loc[:, None])[:, :, None, None]
        k_cache = jnp.where(valid_pos, jnp.stack(k_new), k_buf)
        v_cache = jnp.where(valid_pos, jnp.stack(v_new), v_buf)
        w_query, w_key, w_value = split_qkv(qkv_cols, kv_local, head_dim)
        return (layer_out, k_cache, v_cache, w_query, w_key, w_value, settled['o'], settled['gate'], settled['up'], settled['down'])

    batch_spec = P(('part', 'tpb'), None, None)
    len_spec = P(('part', 'tpb'))
    cache_spec = P(('part', 'tpb'), None, 'tpa', None)
    train_cols = P('part', ('tpa', 'tpb'))
    train_rows = P(('part', 'tpa', 'tpb'), None)
    gain_spec = P('part')
    gen_cols = P('part', 'tpa')
    gen_rows = P(('part', 'tpa'), None)
    return jax.shard_map(one_layer, mesh=mesh, in_specs=(batch_spec, len_spec, cache_spec, cache_spec, train_cols, train_rows, train_cols, train_rows, gain_spec, gain_spec), out_specs=(batch_spec, cache_spec, cache_spec, gen_cols, gen_cols, gen_cols, gen_rows, gen_cols, gen_cols, gen_rows), check_vma=False)
```
